32 devices in a mesh: doc: 8 (over z, y), seq: 4 (over x, core).
Axes of the slice: x: 2, y: 2, z: 4, core: 2. Of those that a mesh axis runs over, the one named last changes fastest.
Arguments:
- queries: bfloat16 [16384, 512], P(('doc', 'seq')), parts along dimension 0, may hold values from -5 to 5
- teacher_keys: bfloat16 [16384, 128], P(('doc', 'seq')), parts along dimension 0, may hold values from -5 to 5
- teacher_values: bfloat16 [16384, 128], P(('doc', 'seq')), parts along dimension 0, may hold values from -5 to 5
- beacon_starts: int32 [1024], P(('doc', 'seq')), parts along dimension 0, may hold values from 0 to 511, as said below
Outputs:
- output_gap: bfloat16 [16384, 512], P(('doc', 'seq')), parts along dimension 0
- beacon_key_grad: float32 [1024, 128], P(('doc', 'seq')), parts along dimension 0
- beacon_value_grad: float32 [1024, 128], P(('doc', 'seq')), parts along dimension 0
The draws below stay inside these ranges and needn't reach their ends.
There are 8 independent parts, one for each index of `doc`. The reference program is written for one: setup_inputs(seed, part) draws one part's arguments, and reference() takes and returns one part's arrays. A program takes and returns all parts, laid end to end along the dimension named above; each array names one. Nothing has to cross between parts.
Inputs may be any that keep to these rules, and one draw needn't show every extreme that they name: `beacon_starts`: each aligned block of 32 entries belongs to one shard of 512 tokens: its first entry is 0 and its entries rise strictly.
All inputs are finite; a program needn't handle non-finite values.
Results may differ from the reference program's by a relative error of at most 0.009.
Values may be sent and summed in bfloat16 or wider, within the bound.
A program may use at most 192 MiB of HBM per device.

```python
import jax
import jax.numpy as jnp
from jax import lax

HEAD = 128
H = 4
TOK_DEV = 512
BEAC = 32
TOKENS = 2048
N_SEQ = 4


def drawn(key):
    seq_tokens = TOK_DEV * N_SEQ
    base_key = jax.random.fold_in(key, 401)
    query_key, keys_key = jax.random.split(base_key, 2)
    queries = jnp.clip(1.41 * jax.random.normal(query_key, (seq_tokens, H * HEAD), jnp.float32), -4.5, 4.5)
    teacher_keys = jnp.clip(1.41 * jax.random.normal(keys_key, (seq_tokens, HEAD), jnp.float32), -4.5, 4.5)
    return (queries, teacher_keys)


def draw_queries(key, part):
    return drawn(key)[0].astype(jnp.bfloat16)


def draw_teacher_keys(key, part):
    return drawn(key)[1].astype(jnp.bfloat16)


def draw_beacon_starts(key, part):
    base_key = jax.random.fold_in(key, 733)

    def shard_starts(shard_key):
        picked = jax.random.permutation(shard_key, TOK_DEV - 1)[:BEAC - 1] + 1
        return jnp.concatenate([jnp.zeros((1,), jnp.int32), jnp.sort(picked).astype(jnp.int32)])
    return jax.vmap(shard_starts)(jax.random.split(base_key, N_SEQ)).reshape(N_SEQ * BEAC)


def block_levels(rng, dims, cuts, least, top_value):
    factor_of, own = 1.0, jax.random.fold_in(rng, 6)
    for axis_at, blocks in cuts:
        draws = jnp.exp(jax.random.uniform(jax.random.fold_in(own, axis_at), (blocks,), jnp.float32, least / len(cuts), top_value / len(cuts)))
        factor_of = factor_of * jnp.repeat(draws, dims[axis_at] // blocks).reshape([-1 if axis == axis_at else 1 for axis in range(len(dims))])
    return factor_of


def gaussian(rng, extent, scale, limit, shards=(), kind=jnp.bfloat16):
    drawn = scale * jax.random.normal(rng, extent, jnp.float32)
    if shards:
        drawn = drawn * block_levels(rng, extent, shards, -0.22, 0.18)
    return jnp.clip(drawn, -limit, limit).astype(kind)


def setup_inputs(seed: int = 0, part: int = 0) -> dict:
    seeds = jax.random.split(jax.random.key(seed), 5)
    part_splits = jax.random.split(jax.random.fold_in(seeds[4], part), 5)
    return {
        "queries": draw_queries(jax.random.fold_in(jax.random.fold_in(seeds[4], part), 71), part),
        "teacher_keys": draw_teacher_keys(jax.random.fold_in(jax.random.fold_in(seeds[4], part), 71), part),
        "teacher_values": gaussian(part_splits[2], (TOKENS, HEAD), 1.0, 5.0, ((0, 4),)),
        "beacon_starts": draw_beacon_starts(jax.random.fold_in(jax.random.fold_in(seeds[4], part), 71), part),
    }


def pooled_beacons(teacher_keys, teacher_values, beacon_starts):
    positions = jnp.arange(TOK_DEV, dtype=jnp.int32)
    firsts = beacon_starts.reshape(N_SEQ, BEAC)
    endings = jnp.concatenate([firsts[:, 1:], jnp.full((N_SEQ, 1), TOK_DEV, jnp.int32)], axis=1)
    member = ((positions[None, None, :] >= firsts[:, :, None]) & (positions[None, None, :] < endings[:, :, None])).astype(jnp.float32)
    counts = jnp.sum(member, axis=2)
    joined = jnp.concatenate([teacher_keys, teacher_values], axis=1).astype(jnp.float32).reshape(N_SEQ, TOK_DEV, 2 * HEAD)
    pooled_sums = jnp.einsum("sbt,std->sbd", member, joined)
    return (pooled_sums / counts[:, :, None]).astype(jnp.bfloat16).reshape(N_SEQ * BEAC, 2 * HEAD)


def reference(queries, teacher_keys, teacher_values, beacon_starts):
    scaling = HEAD ** -0.5
    beacons = pooled_beacons(teacher_keys, teacher_values, beacon_starts)
    beacon_count = N_SEQ * BEAC
    owners = jnp.arange(beacon_count, dtype=jnp.int32) // BEAC
    seq_tokens = TOK_DEV * N_SEQ
    row_count = TOK_DEV * H
    local_pos = jnp.arange(row_count, dtype=jnp.int32) // H
    key_index = jnp.arange(seq_tokens, dtype=jnp.int32)
    positions = jnp.arange(TOK_DEV, dtype=jnp.int32)

    def shard_step(carried, shard_index):
        first_token = shard_index * TOK_DEV
        query_rows = lax.dynamic_slice_in_dim(queries, first_token, TOK_DEV, 0).reshape(row_count, HEAD)
        scores = jnp.dot(query_rows, teacher_keys.T, preferred_element_type=jnp.float32) * scaling
        scores = jnp.where(key_index[None, :] <= (first_token + local_pos)[:, None], scores, -jnp.inf)
        weights = jnp.exp(scores - jnp.max(scores, axis=1, keepdims=True))
        teacher = jnp.dot(weights.astype(jnp.bfloat16), teacher_values, preferred_element_type=jnp.float32) / jnp.sum(weights, axis=1, keepdims=True)
        local_keys = lax.dynamic_slice_in_dim(teacher_keys, first_token, TOK_DEV, 0)
        local_values = lax.dynamic_slice_in_dim(teacher_values, first_token, TOK_DEV, 0)
        keys_all = jnp.concatenate([beacons[:, :HEAD], local_keys], axis=0)
        values_all = jnp.concatenate([beacons[:, HEAD:], local_values], axis=0)
        visible = jnp.concatenate([jnp.broadcast_to(owners[None, :] < shard_index, (row_count, beacon_count)), positions[None, :] <= local_pos[:, None]], axis=1)
        student_scores = jnp.where(visible, jnp.dot(query_rows, keys_all.T, preferred_element_type=jnp.float32) * scaling, -jnp.inf)
        student_weights = jnp.exp(student_scores - jnp.max(student_scores, axis=1, keepdims=True))
        student_probs = student_weights / jnp.sum(student_weights, axis=1, keepdims=True)
        probs_low = student_probs.astype(jnp.bfloat16)
        student = jnp.dot(probs_low, values_all, preferred_element_type=jnp.float32)
        output_gap = (student - teacher).astype(jnp.bfloat16)
        prob_grad = jnp.dot(output_gap, values_all.T, preferred_element_type=jnp.float32)
        row_dot = jnp.sum(student_probs * prob_grad, axis=1, keepdims=True)
        score_grad = (student_probs * (prob_grad - row_dot)).astype(jnp.bfloat16)
        grad_keys = jnp.dot(score_grad[:, :beacon_count].T, query_rows, preferred_element_type=jnp.float32) * scaling
        grad_values = jnp.dot(probs_low[:, :beacon_count].T, output_gap, preferred_element_type=jnp.float32)
        return carried + jnp.concatenate([grad_keys, grad_values], axis=1), output_gap.reshape(TOK_DEV, H * HEAD)

    initial = jnp.zeros((beacon_count, 2 * HEAD), jnp.float32)
    grads, gaps = lax.scan(shard_step, initial, jnp.arange(N_SEQ, dtype=jnp.int32))
    return (gaps.reshape(seq_tokens, H * HEAD), grads[:, :HEAD], grads[:, HEAD:])
```

```python
import functools
import math

import jax
import jax.numpy as jnp
from jax import lax
from jax.experimental import pallas as pl
from jax.experimental.pallas import tpu as pltpu
from jax.sharding import PartitionSpec as P

NEG = -1e30
MESH = pl.DeviceIdType.MESH


def dot_nt(a, b):
    return lax.dot_general(a, b, (((1,), (1,)), ((), ())), preferred_element_type=jnp.float32)


def dot_tn(a, b):
    return lax.dot_general(a, b, (((0,), (0,)), ((), ())), preferred_element_type=jnp.float32)


def dot_nn(a, b):
    return jnp.dot(a, b, preferred_element_type=jnp.float32)


def wide(a, width):
    reps = width // a.shape[1]
    return a if reps == 1 else jnp.concatenate([a] * reps, axis=1)


def with_ones(v):
    return jnp.concatenate([v, jnp.ones_like(v)], axis=1)


def kernel(
    n,
    starts_ref,
    q_ref,
    k_ref,
    v_ref,
    gap_ref,
    gk_ref,
    gv_ref,
    k_all,
    v_all,
    beac,
    state_m,
    state_acc,
    student,
    probs,
    sum_k,
    sum_v,
    stage,
    landed,
    k_send,
    v_send,
    k_fwd,
    v_fwd,
    k_recv,
    v_recv,
    b_send,
    b_recv,
    g_send,
    g_recv,
):
    me = lax.axis_index("seq")
    chip = me // 2
    core = me % 2
    partner = me + 1 - 2 * core
    chips = n // 2
    tok, dim = k_ref.shape
    heads = q_ref.shape[1] // dim
    count = starts_ref.shape[0]
    half = tok // 2
    scaling = dim ** (-0.5)
    fold = scaling * math.log2(math.e)

    def remote(src, dst, send, recv, target):
        return pltpu.make_async_remote_copy(
            src_ref=src,
            dst_ref=dst,
            send_sem=send,
            recv_sem=recv,
            device_id={"seq": target},
            device_id_type=MESH,
        )

    barrier = pltpu.get_barrier_semaphore()
    for other in range(1, n):
        pl.semaphore_signal(
            barrier, inc=1, device_id={"seq": lax.rem(me + other, n)}, device_id_type=MESH
        )

    pos = lax.broadcasted_iota(jnp.int32, (8, tok), 1)
    rank = jnp.zeros((8, tok), jnp.int32)
    for b in range(1, count):
        rank = rank + (pos >= starts_ref[b]).astype(jnp.int32)
    rank = jnp.concatenate([rank] * (count // 8), axis=0)
    member = (rank == lax.broadcasted_iota(jnp.int32, (count, tok), 0)).astype(jnp.float32)
    counts = jnp.sum(member, axis=1, keepdims=True)
    joined = jnp.concatenate([k_ref[...], v_ref[...]], axis=1)
    pooled = dot_nn(member.astype(jnp.bfloat16), joined)
    beac[pl.ds(me, 1)] = (pooled / counts).astype(jnp.bfloat16)[None]

    pl.semaphore_wait(barrier, n - 1)

    def kv_copies(src_k, src_v, slot, sk, sv, target):
        return (
            remote(src_k, k_all.at[slot], sk, k_recv.at[slot], target),
            remote(src_v, v_all.at[slot], sv, v_recv.at[slot], target),
        )

    def direct(c):
        return kv_copies(k_ref, v_ref, me, k_send.at[c], v_send.at[c], 2 * c + core)

    def to_partner():
        return kv_copies(k_ref, v_ref, me, k_send.at[chips], v_send.at[chips], partner)

    def forward(c):
        slot = 2 * c + core
        return kv_copies(k_all.at[slot], v_all.at[slot], slot, k_fwd.at[c], v_fwd.at[c], partner)

    def beacon_copy(s):
        return remote(beac.at[me], beac.at[me], b_send.at[s], b_recv.at[me], s)

    def beacon_arrival(s):
        return remote(beac.at[s], beac.at[s], b_send.at[s], b_recv.at[s], partner)

    def grad_copy(s):
        return remote(stage.at[s], landed.at[me], g_send.at[s], g_recv.at[me], s)

    def grad_arrival(d):
        return remote(stage.at[d], landed.at[d], g_send.at[d], g_recv.at[d], partner)

    for c in range(chips):

        @pl.when(c > chip)
        def _():
            for copy in direct(c):
                copy.start()

    for s in range(1, n):

        @pl.when(s > me)
        def _():
            beacon_copy(s).start()

    @pl.when(core == 0)
    def _():
        for copy in to_partner():
            copy.start()

    def own_tile(h, carry):
        cols = pl.ds(pl.multiple_of(h * dim, dim), dim)
        for part in range(2):
            keys = half * (part + 1)
            rows = pl.ds(part * half, half)
            s = dot_nt(q_ref[rows, cols], k_ref[:keys])
            row_pos = lax.broadcasted_iota(jnp.int32, (half, keys), 0) + part * half
            s = jnp.where(lax.broadcasted_iota(jnp.int32, (half, keys), 1) <= row_pos, s, NEG)
            m = jnp.broadcast_to(jnp.max(s, axis=1, keepdims=True), (half, dim))
            p = jnp.exp2((s - wide(m, keys)) * fold).astype(jnp.bfloat16)
            state_m[h, rows] = m
            state_acc[h, rows] = dot_nn(p, with_ones(v_ref[:keys]))
        return carry

    lax.fori_loop(0, heads, own_tile, 0)

    for s in range(n - 1):

        @pl.when(s < me)
        def _():
            beacon_arrival(s).wait_recv()

        @pl.when(s > me)
        def _():
            beac[s] = jnp.zeros((count, 2 * dim), jnp.bfloat16)

    @pl.when(me < n - 1)
    def _():
        beac[n - 1] = jnp.zeros((count, 2 * dim), jnp.bfloat16)

    nb = n * count

    def student_tile(h, carry):
        cols = pl.ds(pl.multiple_of(h * dim, dim), dim)
        rows = beac[...].reshape(nb, 2 * dim)
        s = dot_nt(q_ref[:, cols], rows[:, :dim])
        s = jnp.where(lax.broadcasted_iota(jnp.int32, (tok, nb), 1) < me * count, s, NEG)
        m_own = state_m[h]
        m = jnp.maximum(m_own, jnp.broadcast_to(jnp.max(s, axis=1, keepdims=True), (tok, dim)))
        w = jnp.exp2((s - wide(m, nb)) * fold)
        acc = state_acc[h] * wide(jnp.exp2((m_own - m) * fold), 2 * dim)
        acc = acc + dot_nn(w.astype(jnp.bfloat16), with_ones(rows[:, dim:]))
        inverse = 1.0 / acc[:, dim:]
        student[h] = acc[:, :dim] * inverse
        probs[h] = (w * wide(inverse, nb)).astype(jnp.bfloat16)
        return carry

    lax.fori_loop(0, heads, student_tile, 0)

    def fold_block(slot):
        def tile(h, carry):
            cols = pl.ds(pl.multiple_of(h * dim, dim), dim)
            s = dot_nt(q_ref[:, cols], k_all[slot])
            m_old = state_m[h]
            m = jnp.maximum(m_old, jnp.broadcast_to(jnp.max(s, axis=1, keepdims=True), (tok, dim)))
            p = jnp.exp2((s - wide(m, tok)) * fold).astype(jnp.bfloat16)
            state_m[h] = m
            state_acc[h] = state_acc[h] * wide(jnp.exp2((m_old - m) * fold), 2 * dim) + dot_nn(
                p, with_ones(v_all[slot])
            )
            return carry

        lax.fori_loop(0, heads, tile, 0)

    @pl.when(core == 1)
    def _():
        for copy in kv_copies(
            k_ref, v_ref, me - 1, k_send.at[chips], v_send.at[chips], partner
        ):
            copy.wait_recv()

    def relay(c, carry):
        arrival = kv_copies(
            k_ref, v_ref, 2 * c + core, k_send.at[c], v_send.at[c], partner
        )
        passed = forward(c)
        for a, f in zip(arrival, passed):
            a.wait_recv()
            f.start()
        return carry

    def direct_block(c, carry):
        fold_block(2 * c + core)
        return carry

    @pl.when(core == 1)
    def _():
        fold_block(me - 1)

    lax.fori_loop(0, chip, relay, 0)
    lax.fori_loop(0, chip, direct_block, 0)

    def passed_block(c, carry):
        slot = 2 * c + 1 - core
        for a in kv_copies(k_ref, v_ref, slot, k_send.at[c], v_send.at[c], partner):
            a.wait_recv()
        fold_block(slot)
        return carry

    lax.fori_loop(0, chip, passed_block, 0)

    sum_k[...] = jnp.zeros_like(sum_k)
    sum_v[...] = jnp.zeros_like(sum_v)

    def grad_tile(h, carry):
        cols = pl.ds(pl.multiple_of(h * dim, dim), dim)
        values = beac[...].reshape(nb, 2 * dim)[:, dim:]
        out = student[h]
        gap = (out - state_acc[h, :, :dim] / state_acc[h, :, dim:]).astype(jnp.bfloat16)
        gap_ref[:, cols] = gap
        row_dot = jnp.sum(out * gap.astype(jnp.float32), axis=1, keepdims=True)
        low = probs[h]
        d = low.astype(jnp.float32) * (dot_nt(gap, values) - row_dot)
        sum_k[...] += dot_tn(d.astype(jnp.bfloat16), q_ref[:, cols])
        sum_v[...] += dot_tn(low, gap)
        return carry

    lax.fori_loop(0, heads, grad_tile, 0)

    terms = jnp.concatenate([sum_k[...] * scaling, sum_v[...]], axis=1)
    stage[...] = terms.astype(jnp.bfloat16).reshape(n, count, 2 * dim)
    for s in range(n - 1):

        @pl.when(s < me)
        def _():
            grad_copy(s).start()

    gk_ref[...] = jnp.zeros_like(gk_ref)
    gv_ref[...] = jnp.zeros_like(gv_ref)
    for d in range(1, n):

        @pl.when(d > me)
        def _():
            grad_arrival(d).wait_recv()
            part = landed[d].astype(jnp.float32)
            gk_ref[...] += part[:, :dim]
            gv_ref[...] += part[:, dim:]

    for c in range(chips):

        @pl.when(c > chip)
        def _():
            for copy in direct(c):
                copy.wait_send()

        @pl.when(c < chip)
        def _():
            for copy in forward(c):
                copy.wait_send()

    for s in range(n):

        @pl.when(s > me)
        def _():
            beacon_copy(s).wait_send()

        @pl.when(s < me)
        def _():
            grad_copy(s).wait_send()

    @pl.when(core == 0)
    def _():
        for copy in to_partner():
            copy.wait_send()


def body(n, queries, teacher_keys, teacher_values, beacon_starts):
    tok, dim = teacher_keys.shape
    heads = queries.shape[1] // dim
    count = beacon_starts.shape[0]
    chips = n // 2
    vmem = pl.BlockSpec(memory_space=pltpu.VMEM)
    dma = pltpu.SemaphoreType.DMA
    return pl.pallas_call(
        functools.partial(kernel, n),
        out_shape=(
            jax.ShapeDtypeStruct(queries.shape, jnp.bfloat16),
            jax.ShapeDtypeStruct((count, dim), jnp.float32),
            jax.ShapeDtypeStruct((count, dim), jnp.float32),
        ),
        in_specs=[pl.BlockSpec(memory_space=pltpu.SMEM), vmem, vmem, vmem],
        out_specs=(vmem, vmem, vmem),
        scratch_shapes=[
            pltpu.VMEM((n, tok, dim), jnp.bfloat16),
            pltpu.VMEM((n, tok, dim), jnp.bfloat16),
            pltpu.VMEM((n, count, 2 * dim), jnp.bfloat16),
            pltpu.VMEM((heads, tok, dim), jnp.float32),
            pltpu.VMEM((heads, tok, 2 * dim), jnp.float32),
            pltpu.VMEM((heads, tok, dim), jnp.float32),
            pltpu.VMEM((heads, tok, n * count), jnp.bfloat16),
            pltpu.VMEM((n * count, dim), jnp.float32),
            pltpu.VMEM((n * count, dim), jnp.float32),
            pltpu.VMEM((n, count, 2 * dim), jnp.bfloat16),
            pltpu.VMEM((n, count, 2 * dim), jnp.bfloat16),
            dma((chips + 1,)),
            dma((chips + 1,)),
            dma((chips,)),
            dma((chips,)),
            dma((n,)),
            dma((n,)),
            dma((n,)),
            dma((n,)),
            dma((n,)),
            dma((n,)),
        ],
        compiler_params=pltpu.CompilerParams(collective_id=0, has_side_effects=True),
    )(beacon_starts, queries, teacher_keys, teacher_values)


def solution(mesh):
    spec = P(("doc", "seq"), None)
    return jax.shard_map(
        functools.partial(body, mesh.shape["seq"]),
        mesh=mesh,
        in_specs=(spec, spec, spec, P(("doc", "seq"))),
        out_specs=(spec, spec, spec),
        check_vma=False,
    )
```

```python
import functools
import math

import jax
import jax.numpy as jnp
from jax import lax
from jax.experimental import pallas as pl
from jax.experimental.pallas import tpu as pltpu
from jax.sharding import PartitionSpec as P

NEG = -1e30
CHUNKS = 2
MESH = pl.DeviceIdType.MESH


def dot_nt(a, b):
    return lax.dot_general(a, b, (((1,), (1,)), ((), ())), preferred_element_type=jnp.float32)


def dot_tn(a, b):
    return lax.dot_general(a, b, (((0,), (0,)), ((), ())), preferred_element_type=jnp.float32)


def dot_nn(a, b):
    return jnp.dot(a, b, preferred_element_type=jnp.float32)


def wide(a, width):
    reps = width // a.shape[1]
    return a if reps == 1 else jnp.concatenate([a] * reps, axis=1)


def with_ones(v):
    return jnp.concatenate([v, jnp.ones_like(v)], axis=1)


def kernel(
    n,
    starts_hbm,
    q_hbm,
    k_hbm,
    v_hbm,
    gap_ref,
    gk_ref,
    gv_ref,
    starts_ref,
    q_ref,
    kv,
    beac,
    state_m,
    state_acc,
    student,
    probs,
    stage,
    landed,
    load,
    kv_send,
    kv_fwd,
    kv_recv,
    b_send,
    b_recv,
    g_send,
    g_recv,
):
    me = lax.axis_index("seq")
    chip = me // 2
    core = me % 2
    partner = me + 1 - 2 * core
    chips = n // 2
    tok, dim = k_hbm.shape
    heads = q_hbm.shape[1] // dim
    count = starts_ref.shape[0]
    nb = n * count
    half = tok // 2
    piece = tok // CHUNKS
    scaling = dim ** (-0.5)
    fold = scaling * math.log2(math.e)

    def remote(src, dst, send, recv, target):
        return pltpu.make_async_remote_copy(
            src_ref=src,
            dst_ref=dst,
            send_sem=send,
            recv_sem=recv,
            device_id={"seq": target},
            device_id_type=MESH,
        )

    barrier = pltpu.get_barrier_semaphore()
    for other in range(1, n):
        pl.semaphore_signal(
            barrier, inc=1, device_id={"seq": lax.rem(me + other, n)}, device_id_type=MESH
        )
    loads = (
        pltpu.make_async_copy(k_hbm, kv.at[me, :, pl.ds(0, dim)], load.at[0]),
        pltpu.make_async_copy(v_hbm, kv.at[me, :, pl.ds(dim, dim)], load.at[1]),
        pltpu.make_async_copy(q_hbm, q_ref, load.at[2]),
        pltpu.make_async_copy(starts_hbm, starts_ref, load.at[3]),
    )
    for copy in loads:
        copy.start()

    def part(i):
        return pl.ds(i * piece, piece)

    def direct(c, i):
        here = kv.at[me, part(i)]
        return remote(here, here, kv_send.at[c, i], kv_recv.at[me, i], 2 * c + core)

    def to_partner(i):
        here = kv.at[me, part(i)]
        return remote(here, here, kv_send.at[chips, i], kv_recv.at[me, i], partner)

    def arrival(slot, i):
        there = kv.at[slot, part(i)]
        return remote(there, there, kv_send.at[chips, i], kv_recv.at[slot, i], partner)

    def forward(c, i):
        slot = 2 * c + core
        there = kv.at[slot, part(i)]
        return remote(there, there, kv_fwd.at[c, i], kv_recv.at[slot, i], partner)

    def beacon_copy(s):
        return remote(beac.at[me], beac.at[me], b_send.at[s], b_recv.at[me], s)

    def beacon_arrival(s):
        return remote(beac.at[s], beac.at[s], b_send.at[s], b_recv.at[s], partner)

    def grad_copy(s):
        return remote(stage.at[s], landed.at[me], g_send.at[s], g_recv.at[me], s)

    def grad_arrival(d):
        return remote(stage.at[d], landed.at[d], g_send.at[d], g_recv.at[d], partner)

    loads[0].wait()
    loads[1].wait()
    pl.semaphore_wait(barrier, n - 1)

    for c in range(1, chips):

        @pl.when(c > chip)
        def _():
            for i in range(CHUNKS):
                direct(c, i).start()

    @pl.when(core == 0)
    def _():
        for i in range(CHUNKS):
            to_partner(i).start()

    loads[3].wait()
    pos = lax.broadcasted_iota(jnp.int32, (8, tok), 1)
    rank = jnp.zeros((8, tok), jnp.int32)
    for b in range(1, count):
        rank = rank + (pos >= starts_ref[b]).astype(jnp.int32)
    rank = jnp.concatenate([rank] * (count // 8), axis=0)
    member = (rank == lax.broadcasted_iota(jnp.int32, (count, tok), 0)).astype(jnp.float32)
    inverse_count = 1.0 / jnp.sum(member, axis=1, keepdims=True)
    pooled = dot_nn(member.astype(jnp.bfloat16), kv[me])
    beac[pl.ds(me, 1)] = (pooled * inverse_count).astype(jnp.bfloat16)[None]

    for s in range(1, n):

        @pl.when(s > me)
        def _():
            beacon_copy(s).start()
            beac[s] = jnp.zeros((count, 2 * dim), jnp.bfloat16)

    loads[2].wait()

    for h in range(heads):
        cols = pl.ds(h * dim, dim)
        for side in range(2):
            keys = half * (side + 1)
            rows = pl.ds(side * half, half)
            s = dot_nt(q_ref[rows, cols], kv[me, :keys, :dim])
            row_pos = lax.broadcasted_iota(jnp.int32, (half, keys), 0) + side * half
            s = jnp.where(lax.broadcasted_iota(jnp.int32, (half, keys), 1) <= row_pos, s, NEG)
            m = jnp.broadcast_to(jnp.max(s, axis=1, keepdims=True), (half, dim))
            p = jnp.exp2((s - wide(m, keys)) * fold).astype(jnp.bfloat16)
            state_m[h, rows] = m
            state_acc[h, rows] = dot_nn(p, with_ones(kv[me, :keys, dim:]))

    for s in range(n - 1):

        @pl.when(s < me)
        def _():
            beacon_arrival(s).wait_recv()

    beacons = beac[...].reshape(nb, 2 * dim)
    for h in range(heads):
        cols = pl.ds(h * dim, dim)
        s = dot_nt(q_ref[:, cols], beacons[:, :dim])
        s = jnp.where(lax.broadcasted_iota(jnp.int32, (tok, nb), 1) < me * count, s, NEG)
        m_own = state_m[h]
        m = jnp.maximum(m_own, jnp.broadcast_to(jnp.max(s, axis=1, keepdims=True), (tok, dim)))
        w = jnp.exp2((s - wide(m, nb)) * fold)
        acc = state_acc[h] * wide(jnp.exp2((m_own - m) * fold), 2 * dim)
        acc = acc + dot_nn(w.astype(jnp.bfloat16), with_ones(beacons[:, dim:]))
        inverse = 1.0 / acc[:, dim:]
        student[h] = acc[:, :dim] * inverse
        probs[h] = (w * wide(inverse, nb)).astype(jnp.bfloat16)

    def fold_block(slot, first, keys):
        for h in range(heads):
            cols = pl.ds(h * dim, dim)
            for side in range(2):
                rows = pl.ds(side * half, half)
                s = dot_nt(q_ref[rows, cols], kv[slot, pl.ds(first, keys), :dim])
                m_old = state_m[h, rows]
                m = jnp.maximum(
                    m_old, jnp.broadcast_to(jnp.max(s, axis=1, keepdims=True), (half, dim))
                )
                p = jnp.exp2((s - wide(m, keys)) * fold).astype(jnp.bfloat16)
                state_m[h, rows] = m
                state_acc[h, rows] = state_acc[h, rows] * wide(
                    jnp.exp2((m_old - m) * fold), 2 * dim
                ) + dot_nn(p, with_ones(kv[slot, pl.ds(first, keys), dim:]))

    @pl.when(core == 1)
    def _():
        for i in range(CHUNKS):
            arrival(me - 1, i).wait_recv()
        fold_block(me - 1, 0, tok)

    def direct_block(c, carry):
        for i in range(CHUNKS):
            arrival(2 * c + core, i).wait_recv()
            forward(c, i).start()
            fold_block(2 * c + core, i * piece, piece)
        return carry

    lax.fori_loop(0, chip, direct_block, 0)

    def passed_block(c, carry):
        slot = 2 * c + 1 - core
        for i in range(CHUNKS):
            arrival(slot, i).wait_recv()
        fold_block(slot, 0, tok)
        return carry

    lax.fori_loop(0, chip, passed_block, 0)

    values = beac[...].reshape(nb, 2 * dim)[:, dim:]
    sum_k = jnp.zeros((nb, dim), jnp.float32)
    sum_v = jnp.zeros((nb, dim), jnp.float32)
    for h in range(heads):
        cols = pl.ds(h * dim, dim)
        out = student[h]
        gap = (out - state_acc[h, :, :dim] / state_acc[h, :, dim:]).astype(jnp.bfloat16)
        gap_ref[:, cols] = gap
        row_dot = jnp.sum(out * gap.astype(jnp.float32), axis=1, keepdims=True)
        low = probs[h]
        d = low.astype(jnp.float32) * (dot_nt(gap, values) - row_dot)
        sum_k += dot_tn(d.astype(jnp.bfloat16), q_ref[:, cols])
        sum_v += dot_tn(low, gap)

    terms = jnp.concatenate([sum_k * scaling, sum_v], axis=1)
    stage[...] = terms.astype(jnp.bfloat16).reshape(n, count, 2 * dim)
    for s in range(n - 1):

        @pl.when(s < me)
        def _():
            grad_copy(s).start()

    gk_ref[...] = jnp.zeros_like(gk_ref)
    gv_ref[...] = jnp.zeros_like(gv_ref)
    for d in range(1, n):

        @pl.when(d > me)
        def _():
            grad_arrival(d).wait_recv()
            term = landed[d].astype(jnp.float32)
            gk_ref[...] += term[:, :dim]
            gv_ref[...] += term[:, dim:]

    for c in range(chips):

        @pl.when(c > chip)
        def _():
            for i in range(CHUNKS):
                direct(c, i).wait_send()

        @pl.when(c < chip)
        def _():
            for i in range(CHUNKS):
                forward(c, i).wait_send()

    for s in range(n):

        @pl.when(s > me)
        def _():
            beacon_copy(s).wait_send()

        @pl.when(s < me)
        def _():
            grad_copy(s).wait_send()

    @pl.when(core == 0)
    def _():
        for i in range(CHUNKS):
            to_partner(i).wait_send()


def hand_out(gap, gk, gv, gap_out, gk_out, gv_out, sems):
    copies = [
        pltpu.make_async_copy(src, dst, sems.at[i])
        for i, (src, dst) in enumerate(((gap, gap_out), (gk, gk_out), (gv, gv_out)))
    ]
    for copy in copies:
        copy.start()
    for copy in copies:
        copy.wait()


def body(n, queries, teacher_keys, teacher_values, beacon_starts):
    tok, dim = teacher_keys.shape
    heads = queries.shape[1] // dim
    count = beacon_starts.shape[0]
    chips = n // 2
    vmem = pl.BlockSpec(memory_space=pltpu.VMEM)
    hbm = pl.BlockSpec(memory_space=pltpu.HBM)
    dma = pltpu.SemaphoreType.DMA
    out_shape = (
        jax.ShapeDtypeStruct(queries.shape, jnp.bfloat16),
        jax.ShapeDtypeStruct((count, dim), jnp.float32),
        jax.ShapeDtypeStruct((count, dim), jnp.float32),
    )
    arrays = [
        pltpu.with_memory_space_constraint(a, pltpu.HBM)
        for a in (beacon_starts, queries, teacher_keys, teacher_values)
    ]
    results = pl.pallas_call(
        functools.partial(kernel, n),
        out_shape=out_shape,
        in_specs=[hbm, hbm, hbm, hbm],
        out_specs=(vmem, vmem, vmem),
        scratch_shapes=[
            pltpu.SMEM((count,), jnp.int32),
            pltpu.VMEM(queries.shape, jnp.bfloat16),
            pltpu.VMEM((n, tok, 2 * dim), jnp.bfloat16),
            pltpu.VMEM((n, count, 2 * dim), jnp.bfloat16),
            pltpu.VMEM((heads, tok, dim), jnp.float32),
            pltpu.VMEM((heads, tok, 2 * dim), jnp.float32),
            pltpu.VMEM((heads, tok, dim), jnp.float32),
            pltpu.VMEM((heads, tok, n * count), jnp.bfloat16),
            pltpu.VMEM((n, count, 2 * dim), jnp.bfloat16),
            pltpu.VMEM((n, count, 2 * dim), jnp.bfloat16),
            dma((4,)),
            dma((chips + 1, CHUNKS)),
            dma((chips, CHUNKS)),
            dma((n, CHUNKS)),
            dma((n,)),
            dma((n,)),
            dma((n,)),
            dma((n,)),
        ],
        compiler_params=pltpu.CompilerParams(
            collective_id=0, has_side_effects=True, vmem_limit_bytes=44 * 2**20
        ),
    )(*arrays)
    return pl.pallas_call(
        hand_out,
        out_shape=out_shape,
        in_specs=[vmem, vmem, vmem],
        out_specs=(hbm, hbm, hbm),
        scratch_shapes=[dma((3,))],
        compiler_params=pltpu.CompilerParams(vmem_limit_bytes=4 * 2**20),
    )(*results)


def solution(mesh):
    spec = P(("doc", "seq"), None)
    return jax.shard_map(
        functools.partial(body, mesh.shape["seq"]),
        mesh=mesh,
        in_specs=(spec, spec, spec, P(("doc", "seq"))),
        out_specs=(spec, spec, spec),
        check_vma=False,
    )
```

```python
import functools
import math

import jax
import jax.numpy as jnp
from jax import lax
from jax.experimental import pallas as pl
from jax.experimental.pallas import tpu as pltpu
from jax.sharding import PartitionSpec as P

NEG = -1e30
CHUNKS = 2
MESH = pl.DeviceIdType.MESH


def dot_nt(a, b):
    return lax.dot_general(a, b, (((1,), (1,)), ((), ())), preferred_element_type=jnp.float32)


def dot_tn(a, b):
    return lax.dot_general(a, b, (((0,), (0,)), ((), ())), preferred_element_type=jnp.float32)


def dot_nn(a, b):
    return jnp.dot(a, b, preferred_element_type=jnp.float32)


def wide(a, width):
    reps = width // a.shape[1]
    return a if reps == 1 else jnp.concatenate([a] * reps, axis=1)


def with_ones(v):
    return jnp.concatenate([v, jnp.ones_like(v)], axis=1)


def kernel(
    n,
    starts_hbm,
    q_hbm,
    k_hbm,
    v_hbm,
    gap_ref,
    gk_ref,
    gv_ref,
    starts_ref,
    q_ref,
    kv,
    beac,
    state_m,
    state_acc,
    own_m,
    own_acc,
    student,
    probs,
    stage,
    landed,
    load,
    kv_send,
    kv_fwd,
    kv_recv,
    b_send,
    b_recv,
    g_send,
    g_recv,
):
    me = lax.axis_index("seq")
    chip = me // 2
    core = me % 2
    partner = me + 1 - 2 * core
    chips = n // 2
    tok, dim = k_hbm.shape
    heads = q_hbm.shape[1] // dim
    count = starts_ref.shape[0]
    nb = n * count
    half = tok // 2
    piece = tok // CHUNKS
    scaling = dim ** (-0.5)
    fold = scaling * math.log2(math.e)

    def remote(src, dst, send, recv, target):
        return pltpu.make_async_remote_copy(
            src_ref=src,
            dst_ref=dst,
            send_sem=send,
            recv_sem=recv,
            device_id={"seq": target},
            device_id_type=MESH,
        )

    barrier = pltpu.get_barrier_semaphore()
    for other in range(1, n):
        pl.semaphore_signal(
            barrier, inc=1, device_id={"seq": lax.rem(me + other, n)}, device_id_type=MESH
        )
    loads = (
        pltpu.make_async_copy(k_hbm, kv.at[me, :, pl.ds(0, dim)], load.at[0]),
        pltpu.make_async_copy(v_hbm, kv.at[me, :, pl.ds(dim, dim)], load.at[1]),
        pltpu.make_async_copy(q_hbm, q_ref, load.at[2]),
        pltpu.make_async_copy(starts_hbm, starts_ref, load.at[3]),
    )
    for copy in loads:
        copy.start()

    def part(i):
        return pl.ds(i * piece, piece)

    def direct(c, i):
        here = kv.at[me, part(i)]
        return remote(here, here, kv_send.at[c, i], kv_recv.at[me, i], 2 * c + core)

    def to_partner(i):
        here = kv.at[me, part(i)]
        return remote(here, here, kv_send.at[chips, i], kv_recv.at[me, i], partner)

    def arrival(slot, i):
        there = kv.at[slot, part(i)]
        return remote(there, there, kv_send.at[chips, i], kv_recv.at[slot, i], partner)

    def forward(c, i):
        slot = 2 * c + core
        there = kv.at[slot, part(i)]
        return remote(there, there, kv_fwd.at[c, i], kv_recv.at[slot, i], partner)

    def beacon_copy(s):
        return remote(beac.at[me], beac.at[me], b_send.at[s], b_recv.at[me], s)

    def beacon_arrival(s):
        return remote(beac.at[s], beac.at[s], b_send.at[s], b_recv.at[s], partner)

    def grad_copy(s):
        return remote(stage.at[s], landed.at[me], g_send.at[s], g_recv.at[me], s)

    def grad_arrival(d):
        return remote(stage.at[d], landed.at[d], g_send.at[d], g_recv.at[d], partner)

    loads[0].wait()
    loads[1].wait()
    pl.semaphore_wait(barrier, n - 1)

    for c in range(1, chips):

        @pl.when(c > chip)
        def _():
            direct(c, 0).start()

    @pl.when(core == 0)
    def _():
        for i in range(CHUNKS):
            to_partner(i).start()

    loads[3].wait()
    pos = lax.broadcasted_iota(jnp.int32, (8, tok), 1)
    rank = jnp.zeros((8, tok), jnp.int32)
    for b in range(1, count):
        rank = rank + (pos >= starts_ref[b]).astype(jnp.int32)
    rank = jnp.concatenate([rank] * (count // 8), axis=0)
    member = (rank == lax.broadcasted_iota(jnp.int32, (count, tok), 0)).astype(jnp.float32)
    inverse_count = 1.0 / jnp.sum(member, axis=1, keepdims=True)
    pooled = dot_nn(member.astype(jnp.bfloat16), kv[me])
    beac[pl.ds(me, 1)] = (pooled * inverse_count).astype(jnp.bfloat16)[None]

    for s in range(1, n):

        @pl.when(s > me)
        def _():
            beacon_copy(s).start()
            beac[s] = jnp.zeros((count, 2 * dim), jnp.bfloat16)

    for c in range(1, chips):

        @pl.when(c > chip)
        def _():
            for i in range(1, CHUNKS):
                direct(c, i).start()

    loads[2].wait()

    for h in range(heads):
        cols = pl.ds(h * dim, dim)
        for side in range(2):
            keys = half * (side + 1)
            rows = pl.ds(side * half, half)
            s = dot_nt(q_ref[rows, cols], kv[me, :keys, :dim])
            row_pos = lax.broadcasted_iota(jnp.int32, (half, keys), 0) + side * half
            s = jnp.where(lax.broadcasted_iota(jnp.int32, (half, keys), 1) <= row_pos, s, NEG)
            m = jnp.broadcast_to(jnp.max(s, axis=1, keepdims=True), (half, dim))
            p = jnp.exp2((s - wide(m, keys)) * fold).astype(jnp.bfloat16)
            acc = dot_nn(p, with_ones(kv[me, :keys, dim:]))
            state_m[h, rows] = m
            state_acc[h, rows] = acc
            own_m[h, rows] = m
            own_acc[h, rows] = acc

    def fold_block(slot, first, keys):
        for h in range(heads):
            cols = pl.ds(h * dim, dim)
            for side in range(2):
                rows = pl.ds(side * half, half)
                s = dot_nt(q_ref[rows, cols], kv[slot, pl.ds(first, keys), :dim])
                m_old = state_m[h, rows]
                m = jnp.maximum(
                    m_old, jnp.broadcast_to(jnp.max(s, axis=1, keepdims=True), (half, dim))
                )
                p = jnp.exp2((s - wide(m, keys)) * fold).astype(jnp.bfloat16)
                state_m[h, rows] = m
                state_acc[h, rows] = state_acc[h, rows] * wide(
                    jnp.exp2((m_old - m) * fold), 2 * dim
                ) + dot_nn(p, with_ones(kv[slot, pl.ds(first, keys), dim:]))

    @pl.when(core == 1)
    def _():
        for i in range(CHUNKS):
            arrival(me - 1, i).wait_recv()
        fold_block(me - 1, 0, tok)

    def direct_piece(c, i):
        arrival(2 * c + core, i).wait_recv()
        forward(c, i).start()
        fold_block(2 * c + core, i * piece, piece)

    def passed_piece(c, i):
        arrival(2 * c + 1 - core, i).wait_recv()
        fold_block(2 * c + 1 - core, i * piece, piece)

    @pl.when(chip > 0)
    def _():
        direct_piece(0, 0)

    for s in range(n - 1):

        @pl.when(s < me)
        def _():
            beacon_arrival(s).wait_recv()

    beacons = beac[...].reshape(nb, 2 * dim)
    for h in range(heads):
        cols = pl.ds(h * dim, dim)
        s = dot_nt(q_ref[:, cols], beacons[:, :dim])
        s = jnp.where(lax.broadcasted_iota(jnp.int32, (tok, nb), 1) < me * count, s, NEG)
        m_own = own_m[h]
        m = jnp.maximum(m_own, jnp.broadcast_to(jnp.max(s, axis=1, keepdims=True), (tok, dim)))
        w = jnp.exp2((s - wide(m, nb)) * fold)
        acc = own_acc[h] * wide(jnp.exp2((m_own - m) * fold), 2 * dim)
        acc = acc + dot_nn(w.astype(jnp.bfloat16), with_ones(beacons[:, dim:]))
        inverse = 1.0 / acc[:, dim:]
        student[h] = acc[:, :dim] * inverse
        probs[h] = (w * wide(inverse, nb)).astype(jnp.bfloat16)

    @pl.when(chip > 0)
    def _():
        passed_piece(0, 0)
        for i in range(1, CHUNKS):
            direct_piece(0, i)
            passed_piece(0, i)

    def earlier_chip(c, carry):
        for i in range(CHUNKS):
            direct_piece(c, i)
            passed_piece(c, i)
        return carry

    if chips > 2:
        lax.fori_loop(1, chip, earlier_chip, 0)

    values = beac[...].reshape(nb, 2 * dim)[:, dim:]
    sum_k = jnp.zeros((nb, dim), jnp.float32)
    sum_v = jnp.zeros((nb, dim), jnp.float32)
    for h in range(heads):
        cols = pl.ds(h * dim, dim)
        out = student[h]
        gap = (out - state_acc[h, :, :dim] / state_acc[h, :, dim:]).astype(jnp.bfloat16)
        gap_ref[:, cols] = gap
        row_dot = jnp.sum(out * gap.astype(jnp.float32), axis=1, keepdims=True)
        low = probs[h]
        d = low.astype(jnp.float32) * (dot_nt(gap, values) - row_dot)
        sum_k += dot_tn(d.astype(jnp.bfloat16), q_ref[:, cols])
        sum_v += dot_tn(low, gap)

    terms = jnp.concatenate([sum_k * scaling, sum_v], axis=1)
    stage[...] = terms.astype(jnp.bfloat16).reshape(n, count, 2 * dim)
    for s in range(n - 1):

        @pl.when(s < me)
        def _():
            grad_copy(s).start()

    gk_ref[...] = jnp.zeros_like(gk_ref)
    gv_ref[...] = jnp.zeros_like(gv_ref)
    for d in range(1, n):

        @pl.when(d > me)
        def _():
            grad_arrival(d).wait_recv()
            term = landed[d].astype(jnp.float32)
            gk_ref[...] += term[:, :dim]
            gv_ref[...] += term[:, dim:]

    for c in range(chips):

        @pl.when(c > chip)
        def _():
            for i in range(CHUNKS):
                direct(c, i).wait_send()

        @pl.when(c < chip)
        def _():
            for i in range(CHUNKS):
                forward(c, i).wait_send()

    for s in range(n):

        @pl.when(s > me)
        def _():
            beacon_copy(s).wait_send()

        @pl.when(s < me)
        def _():
            grad_copy(s).wait_send()

    @pl.when(core == 0)
    def _():
        for i in range(CHUNKS):
            to_partner(i).wait_send()


def hand_out(gap, gk, gv, gap_out, gk_out, gv_out, sems):
    copies = [
        pltpu.make_async_copy(src, dst, sems.at[i])
        for i, (src, dst) in enumerate(((gap, gap_out), (gk, gk_out), (gv, gv_out)))
    ]
    for copy in copies:
        copy.start()
    for copy in copies:
        copy.wait()


def body(n, queries, teacher_keys, teacher_values, beacon_starts):
    tok, dim = teacher_keys.shape
    heads = queries.shape[1] // dim
    count = beacon_starts.shape[0]
    chips = n // 2
    vmem = pl.BlockSpec(memory_space=pltpu.VMEM)
    hbm = pl.BlockSpec(memory_space=pltpu.HBM)
    dma = pltpu.SemaphoreType.DMA
    out_shape = (
        jax.ShapeDtypeStruct(queries.shape, jnp.bfloat16),
        jax.ShapeDtypeStruct((count, dim), jnp.float32),
        jax.ShapeDtypeStruct((count, dim), jnp.float32),
    )
    arrays = [
        pltpu.with_memory_space_constraint(a, pltpu.HBM)
        for a in (beacon_starts, queries, teacher_keys, teacher_values)
    ]
    results = pl.pallas_call(
        functools.partial(kernel, n),
        out_shape=out_shape,
        in_specs=[hbm, hbm, hbm, hbm],
        out_specs=(vmem, vmem, vmem),
        scratch_shapes=[
            pltpu.SMEM((count,), jnp.int32),
            pltpu.VMEM(queries.shape, jnp.bfloat16),
            pltpu.VMEM((n, tok, 2 * dim), jnp.bfloat16),
            pltpu.VMEM((n, count, 2 * dim), jnp.bfloat16),
            pltpu.VMEM((heads, tok, dim), jnp.float32),
            pltpu.VMEM((heads, tok, 2 * dim), jnp.float32),
            pltpu.VMEM((heads, tok, dim), jnp.float32),
            pltpu.VMEM((heads, tok, 2 * dim), jnp.float32),
            pltpu.VMEM((heads, tok, dim), jnp.float32),
            pltpu.VMEM((heads, tok, n * count), jnp.bfloat16),
            pltpu.VMEM((n, count, 2 * dim), jnp.bfloat16),
            pltpu.VMEM((n, count, 2 * dim), jnp.bfloat16),
            dma((4,)),
            dma((chips + 1, CHUNKS)),
            dma((chips, CHUNKS)),
            dma((n, CHUNKS)),
            dma((n,)),
            dma((n,)),
            dma((n,)),
            dma((n,)),
        ],
        compiler_params=pltpu.CompilerParams(
            collective_id=0, has_side_effects=True, vmem_limit_bytes=44 * 2**20
        ),
    )(*arrays)
    return pl.pallas_call(
        hand_out,
        out_shape=out_shape,
        in_specs=[vmem, vmem, vmem],
        out_specs=(hbm, hbm, hbm),
        scratch_shapes=[dma((3,))],
        compiler_params=pltpu.CompilerParams(vmem_limit_bytes=4 * 2**20),
    )(*results)


def solution(mesh):
    spec = P(("doc", "seq"), None)
    return jax.shard_map(
        functools.partial(body, mesh.shape["seq"]),
        mesh=mesh,
        in_specs=(spec, spec, spec, P(("doc", "seq"))),
        out_specs=(spec, spec, spec),
        check_vma=False,
    )
```
